32 devices in a mesh: lev: 4 (over x, core), lon: 8 (over z, y).
Axes of the slice: x: 2, y: 2, z: 4, core: 2. Of those that a mesh axis runs over, the one named last changes fastest.
Arguments:
- previous: float32 [36, 64, 4096], P('lev', None, 'lon'), may hold values from -4 to 4
- loss_matrix: float32 [36, 64, 64], P('lev'), may hold values from -3 to 10, as said below
- pair_matrix: float32 [36, 64, 64], P('lev'), may hold values from -0.1875 to 0.1875
- diffusivity: float32 [36], P('lev'), may hold values from 200 to 2000
- mixing: float32 [36], P('lev'), may hold values from 0.1 to 1
Outputs:
- concentration: float32 [36, 64, 4096], P('lev', None, 'lon')
- level_variance: float32 [36, 64], P('lev')
The draws below stay inside these ranges and needn't reach their ends.
Inputs may be any that keep to these rules, and one draw needn't show every extreme that they name: `loss_matrix`: each of the 36 blocks is symmetric and at least 0.05 times the identity in the positive definite order.
All inputs are finite; a program needn't handle non-finite values.
Results may differ from the reference program's by a relative error of at most 0.00045.
Values sent between devices are 32-bit elements; how exact they have to be, the bound alone decides.
A program may use at most 64 MiB of HBM per device.

```python
import math
import jax
import jax.numpy as jnp
from jax import lax

S = 64
ITERS = 2
L = 36
NCOL = 4096


def draw_loss_matrix(key, part):
    first_key, second_key = jax.random.split(jax.random.fold_in(key, 17))
    base = jax.random.normal(first_key, (L, S, S), jnp.float32)
    level_scale = jax.random.uniform(second_key, (L,), jnp.float32, 0.2, 2.0)
    gram = jnp.einsum('lst,lut->lsu', base, base, precision=lax.Precision.HIGHEST) / S
    gram = 0.5 * (gram + jnp.swapaxes(gram, 1, 2))
    identity = jnp.eye(S, dtype=jnp.float32)
    return level_scale[:, None, None] * (0.25 * identity + gram)


def block_scale(own_key, dims, shards, least, high):
    def one(position, parts):
        steps = jax.random.uniform(jax.random.fold_in(jax.random.fold_in(own_key, 6), position), (parts,), jnp.float32, least / len(shards), high / len(shards))
        return jnp.repeat(jnp.exp(steps), dims[position] // parts).reshape((-1,) + (1,) * (len(dims) - position - 1))

    level = one(*shards[0])
    for cut in shards[1:]:
        level = level * one(*cut)
    return level


def normal_values(own_key, dims, scale, most, cuts=(), held_as=jnp.bfloat16):
    gain = block_scale(own_key, dims, cuts, -0.22, 0.18) if cuts else 1.0
    drawn = jax.random.normal(own_key, dims, jnp.float32) * scale * gain
    return jnp.minimum(jnp.maximum(drawn, -most), most).astype(held_as)


def setup_inputs(seed: int = 0) -> dict:
    key_of = jax.random.split(jax.random.key(seed), 6)
    return {
        "previous": normal_values(key_of[0], (L, S, NCOL), 1.0, 4.0, ((0, 4), (2, 8)), jnp.float32),
        "loss_matrix": draw_loss_matrix(jax.random.fold_in(key_of[5], 71), 0),
        "pair_matrix": normal_values(key_of[2], (L, S, S), (16 * S) ** -0.5, 0.1875, ((0, 4),), jnp.float32),
        "diffusivity": jnp.clip(jnp.exp(math.log(2000.0) - 2.3025851 * jax.random.uniform(key_of[3], (L,), jnp.float32) ** block_scale(key_of[3], (L,), ((0, 4),), -0.2, 0.2)), 200.0, 2000.0),
        "mixing": jnp.clip(jnp.exp(math.log(1.0) - 2.3025851 * jax.random.uniform(key_of[4], (L,), jnp.float32) ** block_scale(key_of[4], (L,), ((0, 4),), -0.2, 0.2)), 0.1, 1.0),
    }


HIGHEST_PRECISION = lax.Precision.HIGHEST

def residual_of(current, previous, loss_matrix, pair_matrix, diffusivity, mixing):
    above_links = jnp.concatenate([jnp.zeros((1,), current.dtype), diffusivity[:-1]])
    zero_level = jnp.zeros_like(current[:1])
    level_above = jnp.concatenate([zero_level, current[:-1]], axis=0)
    level_below = jnp.concatenate([current[1:], zero_level], axis=0)
    across = mixing[:, None, None] * (jnp.roll(current, 1, axis=2) + jnp.roll(current, -1, axis=2) - 2.0 * current)
    own_chem = jnp.einsum('lst,ltc->lsc', loss_matrix, current, precision=HIGHEST_PRECISION)
    pair_chem = jnp.einsum('lst,ltc->lsc', pair_matrix, current * current, precision=HIGHEST_PRECISION)
    vertical = diffusivity[:, None, None] * (current - level_below) + above_links[:, None, None] * (current - level_above)
    return current + own_chem + pair_chem + vertical - across - previous

def newton_solve(forcing, loss_matrix, diffusivity):
    species = loss_matrix.shape[1]
    identity = jnp.eye(species, dtype=loss_matrix.dtype)
    above_links = jnp.concatenate([jnp.zeros((1,), diffusivity.dtype), diffusivity[:-1]])
    diagonal = (1.0 + above_links + diffusivity)[:, None, None] * identity + loss_matrix

    def factor_step(prev_inverse, pieces):
        block, link_above = pieces
        inverse = jnp.linalg.inv(block - link_above * link_above * prev_inverse)
        return (inverse, inverse)
    _, inverses = lax.scan(factor_step, jnp.zeros_like(identity), (diagonal, above_links))

    def forward(prev_lifted, pieces):
        inverse, link_above, right_side = pieces
        lifted = jnp.dot(inverse, right_side + link_above * prev_lifted, precision=HIGHEST_PRECISION)
        return (lifted, lifted)
    _, lifted_all = lax.scan(forward, jnp.zeros_like(forcing[0]), (inverses, above_links, forcing))

    def backward(next_value, pieces):
        inverse, link_below, lifted_level = pieces
        value = lifted_level + link_below * jnp.dot(inverse, next_value, precision=HIGHEST_PRECISION)
        return (value, value)
    _, solution = lax.scan(backward, jnp.zeros_like(forcing[0]), (inverses, diffusivity, lifted_all), reverse=True)
    return solution

def reference(previous, loss_matrix, pair_matrix, diffusivity, mixing):
    current = previous
    for newton_step in range(ITERS):
        forcing = residual_of(current, previous, loss_matrix, pair_matrix, diffusivity, mixing)
        current = current - newton_solve(forcing, loss_matrix, diffusivity)
    variance = jnp.mean(current * current, axis=2)
    return (current, variance)
```

```python
import functools

import jax
import jax.numpy as jnp
from jax import lax
from jax.experimental import pallas as pl
from jax.experimental.pallas import tpu as pltpu
from jax.sharding import PartitionSpec as P

ITERS = 2
HIGHEST = lax.Precision.HIGHEST
SMEM = pl.BlockSpec(memory_space=pltpu.SMEM)
VMEM = pl.BlockSpec(memory_space=pltpu.VMEM)


def dot(a, b, dims=((1,), (0,))):
    return lax.dot_general(
        a, b, (dims, ((), ())), precision=HIGHEST, preferred_element_type=jnp.float32
    )


def dot_t(a, b):
    return dot(a, b, ((1,), (1,)))


def eye_of(size):
    rows = lax.broadcasted_iota(jnp.int32, (size, size), 0)
    cols = lax.broadcasted_iota(jnp.int32, (size, size), 1)
    return rows == cols


def invert_all(blocks):
    size = blocks[0].shape[0]
    on_diag = eye_of(size)
    unit = jnp.where(on_diag, 1.0, 0.0).astype(jnp.float32)
    start, worst = [], None
    for a in blocks:
        total = jnp.sum(jnp.abs(a), axis=0, keepdims=True)
        diag = jnp.sum(jnp.where(on_diag, a, 0.0), axis=0, keepdims=True)
        hi = jnp.max(total)
        lo = jnp.maximum(jnp.min(2.0 * diag - total), 1.0)
        scale = 2.0 / (hi + lo)
        rho = (hi - lo) / (hi + lo)
        start.append(scale * (2.0 * unit - scale * a))
        worst = rho if worst is None else jnp.maximum(worst, rho)

    def go_on(carry):
        return carry[0] > 3e-8

    def step(carry):
        bound, *xs = carry
        rest = [unit - dot(a, x) for a, x in zip(blocks, xs)]
        return (bound * bound, *[x + dot(x, r) for x, r in zip(xs, rest)])

    return lax.while_loop(go_on, step, (worst * worst, *start))[1:]


def plan(lo, hi, out):
    if lo >= hi:
        return 0
    mid = lo + (hi - lo) // 2
    depth = 1 + max(plan(lo, mid, out), plan(mid + 1, hi, out))
    out.setdefault(depth, []).append((lo, mid, hi))
    return depth


def dense_inverse(diag, low):
    count, size = len(diag), diag[0].shape[0]
    unit = jnp.where(eye_of(size), 1.0, 0.0).astype(jnp.float32)
    by_depth, done = {}, {}
    plan(0, count, by_depth)
    for depth in sorted(by_depth):
        nodes = by_depth[depth]
        schur, arms = [], []
        for lo, mid, hi in nodes:
            s, parts = diag[mid], []
            if lo < mid:
                panel = done[lo, mid][-1]
                arm = low_right(panel, low, mid, False)
                s = s - low(mid, arm[-size:])
                parts.append(arm)
            parts.append(unit)
            if mid + 1 < hi:
                panel = done[mid + 1, hi][0]
                arm = low_right(panel, low, mid + 1, True)
                s = s - low(mid + 1, arm[:size], True)
                parts.append(arm)
            schur.append(s)
            arms.append(jnp.concatenate(parts, axis=0) if len(parts) > 1 else parts[0])
        for (lo, mid, hi), v, z in zip(nodes, arms, invert_all(schur)):
            if hi - lo == 1:
                done[lo, hi] = [z]
                continue
            w = dot(v, z)
            panels = []
            for k in range(lo, hi):
                vk = v[(k - lo) * size : (k - lo + 1) * size]
                new = w if k == mid else dot_t(w, vk)
                pieces = []
                for a, b in ((lo, mid), (mid, mid + 1), (mid + 1, hi)):
                    if a >= b:
                        continue
                    piece = new[(a - lo) * size : (b - lo) * size]
                    if a <= k < b and k != mid:
                        piece = piece + done[a, b][k - a]
                    pieces.append(piece)
                panels.append(jnp.concatenate(pieces, axis=0) if len(pieces) > 1 else pieces[0])
            done[lo, hi] = panels
    return done[0, count]


def low_right(panel, low, k, plain):
    return low(k, panel, not plain, True)


def split(x):
    high = x.astype(jnp.bfloat16)
    return high, (x - high.astype(jnp.float32)).astype(jnp.bfloat16)


def dot3(a_high, a_low, b):
    b_high, b_low = split(b)
    mul = functools.partial(jnp.dot, preferred_element_type=jnp.float32)
    return mul(a_high, b_high) + (mul(a_low, b_high) + mul(a_high, b_low))


def factor_kernel(links_ref, loss_ref, high_ref, low_ref, ends_ref, send_ref):
    levels, size = loss_ref.shape[0], loss_ref.shape[1]
    inner = levels - 1
    on_diag = eye_of(size)

    def diag_of(k):
        return loss_ref[k] + jnp.where(on_diag, 1.0 + links_ref[k] + links_ref[k + 1], 0.0)

    def low(k, x, transposed=False, right=False):
        return links_ref[k] * x

    panels = dense_inverse([diag_of(k) for k in range(inner)], low)
    top_link, inner_link = links_ref[0], links_ref[inner]
    for k, panel in enumerate(panels):
        high, rest = split(panel)
        high_ref[:, k * size : (k + 1) * size] = high
        low_ref[:, k * size : (k + 1) * size] = rest
    ends_ref[0] = top_link * panels[0]
    ends_ref[1] = inner_link * panels[-1]
    send_ref[0] = diag_of(inner) - inner_link * inner_link * panels[-1][-size:]
    send_ref[1] = top_link * top_link * panels[0][:size]
    send_ref[2] = inner_link * top_link * panels[0][-size:]


def interface_kernel(place_ref, all_ref, ends_ref, high_ref, low_ref, rows_ref):
    count, size = all_ref.shape[0], all_ref.shape[2]
    diag = [
        all_ref[k, 0] - all_ref[k + 1, 1] if k + 1 < count else all_ref[k, 0]
        for k in range(count)
    ]

    def low(k, x, transposed=False, right=False):
        block = all_ref[k, 2]
        if right:
            return dot_t(x, block) if transposed else dot(x, block)
        return dot(block, x, ((0,), (0,))) if transposed else dot(block, x)

    for k, panel in enumerate(dense_inverse(diag, low)):
        rows_ref[k] = panel
    me = place_ref[0]
    own = rows_ref[me]
    above = rows_ref[jnp.maximum(me - 1, 0)]
    inner = dot_t(ends_ref[0], above) + dot_t(ends_ref[1], own)
    length = inner.shape[0]
    high_ref[:length], low_ref[:length] = split(inner)
    high_ref[length:], low_ref[length:] = split(own.T)


def forcing_kernel(
    links_ref, mix_ref, cur_ref, left_ref, right_ref, prev_ref, pair_ref, high_ref, low_ref,
    part_ref, side_ref, top_ref, force_ref,
):
    levels, size, columns = cur_ref.shape
    lane = lax.broadcasted_iota(jnp.int32, (size, columns), 1)
    for k in range(levels):
        c = cur_ref[k]
        back = jnp.where(lane == 0, left_ref[k], pltpu.roll(c, 1, 1))
        ahead = jnp.where(lane == columns - 1, right_ref[k], pltpu.roll(c, columns - 1, 1))
        p_high, p_low = split(pair_ref[k])
        chem = dot3(p_high, p_low, c * c)
        force_ref[k * size : (k + 1) * size] = (
            prev_ref[k] - chem + mix_ref[k] * (back + ahead - 2.0 * c)
        )
    inner = (levels - 1) * size
    part = dot3(high_ref[...], low_ref[...], force_ref[:inner])
    part_ref[...] = part
    side_ref[...] = force_ref[inner:] + links_ref[levels - 1] * part[-size:]
    top_ref[...] = links_ref[0] * part[:size]


def finish_kernel(part_ref, sides_ref, high_ref, low_ref, out_ref, sum_ref):
    levels, size, columns = out_ref.shape
    inner = (levels - 1) * size
    x = dot3(high_ref[...], low_ref[...], sides_ref[...])
    for k in range(levels):
        row = x[k * size : (k + 1) * size]
        if k < levels - 1:
            row = row + part_ref[k * size : (k + 1) * size]
        out_ref[k] = row
        sum_ref[k] = jnp.sum(row * row, axis=1, keepdims=True)


def call(kernel, outs, places, scratch=()):
    return pl.pallas_call(
        kernel,
        out_shape=[jax.ShapeDtypeStruct(shape, dtype) for shape, dtype in outs],
        in_specs=places,
        out_specs=[VMEM] * len(outs),
        scratch_shapes=list(scratch),
        compiler_params=pltpu.CompilerParams(vmem_limit_bytes=60 * 2**20),
    )


def local(previous, loss_matrix, pair_matrix, diffusivity, mixing):
    levels, size, columns = previous.shape
    count = lax.axis_size("lev")
    around = lax.axis_size("lon")
    inner = (levels - 1) * size
    f32, bf16 = jnp.float32, jnp.bfloat16
    top_link = lax.ppermute(
        diffusivity[levels - 1 :], "lev", [(i, i + 1) for i in range(count - 1)]
    )
    links = jnp.concatenate([top_link, diffusivity])
    place = lax.axis_index("lev").astype(jnp.int32).reshape(1)
    g_high, g_low, ends, sent = call(
        factor_kernel,
        [((inner, inner), bf16), ((inner, inner), bf16), ((2, inner, size), f32), ((3, size, size), f32)],
        [SMEM, VMEM],
    )(links, loss_matrix)
    gathered = lax.all_gather(sent, "lev", axis=0)
    h_high, h_low = call(
        interface_kernel,
        [((levels * size, count * size), bf16)] * 2,
        [SMEM, VMEM, VMEM],
        [pltpu.VMEM((count, count * size, size), f32)],
    )(place, gathered, ends)
    current = previous
    for _ in range(ITERS):
        left = lax.ppermute(
            current[:, :, columns - 1 :], "lon", [(i, (i + 1) % around) for i in range(around)]
        )
        right = lax.ppermute(
            current[:, :, :1], "lon", [((i + 1) % around, i) for i in range(around)]
        )
        part, side, top = call(
            forcing_kernel,
            [((inner, columns), f32), ((size, columns), f32), ((size, columns), f32)],
            [SMEM, SMEM] + [VMEM] * 7,
            [pltpu.VMEM((levels * size, columns), f32)],
        )(links, mixing, current, left, right, previous, pair_matrix, g_high, g_low)
        side = side + lax.ppermute(top, "lev", [(i + 1, i) for i in range(count - 1)])
        sides = lax.all_gather(side, "lev", axis=0, tiled=True)
        current, squares = call(
            finish_kernel,
            [((levels, size, columns), f32), ((levels, size, 1), f32)],
            [VMEM] * 4,
        )(part, sides, h_high, h_low)
    totals = jnp.sum(lax.all_gather(squares[:, :, 0], "lon", axis=0), axis=0)
    return (current, totals / (columns * around))


def solution(mesh):
    placed = (P("lev", None, "lon"), P("lev", None, None), P("lev", None, None), P("lev"), P("lev"))
    return jax.shard_map(
        local,
        mesh=mesh,
        in_specs=placed,
        out_specs=(P("lev", None, "lon"), P("lev", None)),
        check_vma=False,
    )
```

```python
import functools

import jax
import jax.numpy as jnp
from jax import lax
from jax.experimental import pallas as pl
from jax.experimental.pallas import tpu as pltpu
from jax.sharding import PartitionSpec as P

HIGHEST = lax.Precision.HIGHEST
SMEM = pl.BlockSpec(memory_space=pltpu.SMEM)
VMEM = pl.BlockSpec(memory_space=pltpu.VMEM)


def dot(a, b, dims=((1,), (0,))):
    return lax.dot_general(
        a, b, (dims, ((), ())), precision=HIGHEST, preferred_element_type=jnp.float32
    )


def dot_t(a, b):
    return dot(a, b, ((1,), (1,)))


def eye_of(size):
    rows = lax.broadcasted_iota(jnp.int32, (size, size), 0)
    cols = lax.broadcasted_iota(jnp.int32, (size, size), 1)
    return rows == cols


def invert_all(blocks):
    size = blocks[0].shape[0]
    on_diag = eye_of(size)
    unit = jnp.where(on_diag, 1.0, 0.0).astype(jnp.float32)
    start, worst = [], None
    for a in blocks:
        total = jnp.sum(jnp.abs(a), axis=0, keepdims=True)
        diag = jnp.sum(jnp.where(on_diag, a, 0.0), axis=0, keepdims=True)
        hi = jnp.max(total)
        lo = jnp.maximum(jnp.min(2.0 * diag - total), 1.0)
        scale = 2.0 / (hi + lo)
        rho = (hi - lo) / (hi + lo)
        start.append(scale * (2.0 * unit - scale * a))
        worst = rho if worst is None else jnp.maximum(worst, rho)

    def go_on(carry):
        return carry[0] > 3e-8

    def step(carry):
        bound, *xs = carry
        rest = [unit - dot(a, x) for a, x in zip(blocks, xs)]
        return (bound * bound, *[x + dot(x, r) for x, r in zip(xs, rest)])

    return lax.while_loop(go_on, step, (worst * worst, *start))[1:]


def plan(lo, hi, out):
    if lo >= hi:
        return 0
    mid = lo + (hi - lo) // 2
    depth = 1 + max(plan(lo, mid, out), plan(mid + 1, hi, out))
    out.setdefault(depth, []).append((lo, mid, hi))
    return depth


def dense_inverse(diag, low):
    count, size = len(diag), diag[0].shape[0]
    unit = jnp.where(eye_of(size), 1.0, 0.0).astype(jnp.float32)
    by_depth, done = {}, {}
    plan(0, count, by_depth)
    for depth in sorted(by_depth):
        nodes = by_depth[depth]
        schur, arms = [], []
        for lo, mid, hi in nodes:
            s, parts = diag[mid], []
            if lo < mid:
                panel = done[lo, mid][-1]
                arm = low_right(panel, low, mid, False)
                s = s - low(mid, arm[-size:])
                parts.append(arm)
            parts.append(unit)
            if mid + 1 < hi:
                panel = done[mid + 1, hi][0]
                arm = low_right(panel, low, mid + 1, True)
                s = s - low(mid + 1, arm[:size], True)
                parts.append(arm)
            schur.append(s)
            arms.append(jnp.concatenate(parts, axis=0) if len(parts) > 1 else parts[0])
        for (lo, mid, hi), v, z in zip(nodes, arms, invert_all(schur)):
            if hi - lo == 1:
                done[lo, hi] = [z]
                continue
            w = dot(v, z)
            panels = []
            for k in range(lo, hi):
                vk = v[(k - lo) * size : (k - lo + 1) * size]
                new = w if k == mid else dot_t(w, vk)
                pieces = []
                for a, b in ((lo, mid), (mid, mid + 1), (mid + 1, hi)):
                    if a >= b:
                        continue
                    piece = new[(a - lo) * size : (b - lo) * size]
                    if a <= k < b and k != mid:
                        piece = piece + done[a, b][k - a]
                    pieces.append(piece)
                panels.append(jnp.concatenate(pieces, axis=0) if len(pieces) > 1 else pieces[0])
            done[lo, hi] = panels
    return done[0, count]


def low_right(panel, low, k, plain):
    return low(k, panel, not plain, True)


def split(x):
    high = x.astype(jnp.bfloat16)
    return high, (x - high.astype(jnp.float32)).astype(jnp.bfloat16)


def dot3(a_high, a_low, b):
    b_high, b_low = split(b)
    mul = functools.partial(jnp.dot, preferred_element_type=jnp.float32)
    return mul(a_high, b_high) + (mul(a_low, b_high) + mul(a_high, b_low))


def factor_kernel(links_ref, top_ref, loss_ref, high_ref, low_ref, ends_ref, send_ref):
    levels, size = loss_ref.shape[0], loss_ref.shape[1]
    inner = levels - 1
    on_diag = eye_of(size)
    top_link, inner_link = top_ref[0:1, 0:1], links_ref[inner - 1]

    def diag_of(k):
        above = top_link if k == 0 else links_ref[k - 1]
        return loss_ref[k] + jnp.where(on_diag, 1.0 + above + links_ref[k], 0.0)

    def low(k, x, transposed=False, right=False):
        return links_ref[k - 1] * x

    panels = dense_inverse([diag_of(k) for k in range(inner)], low)
    for k, panel in enumerate(panels):
        high, rest = split(panel)
        high_ref[:, k * size : (k + 1) * size] = high
        low_ref[:, k * size : (k + 1) * size] = rest
    ends_ref[0] = top_link * panels[0]
    ends_ref[1] = inner_link * panels[-1]
    send_ref[0] = diag_of(inner) - inner_link * inner_link * panels[-1][-size:]
    send_ref[1] = top_link * top_link * panels[0][:size]
    send_ref[2] = inner_link * top_link * panels[0][-size:]


def interface_kernel(place_ref, all_ref, ends_ref, high_ref, low_ref, rows_ref):
    count, size = all_ref.shape[0], all_ref.shape[2]
    diag = [
        all_ref[k, 0] - all_ref[k + 1, 1] if k + 1 < count else all_ref[k, 0]
        for k in range(count)
    ]

    def low(k, x, transposed=False, right=False):
        block = all_ref[k, 2]
        if right:
            return dot_t(x, block) if transposed else dot(x, block)
        return dot(block, x, ((0,), (0,))) if transposed else dot(block, x)

    for k, panel in enumerate(dense_inverse(diag, low)):
        rows_ref[k] = panel
    me = place_ref[0]
    own = rows_ref[me]
    above = rows_ref[jnp.maximum(me - 1, 0)]
    inner = dot_t(ends_ref[0], above) + dot_t(ends_ref[1], own)
    length = inner.shape[0]
    high_ref[:length], low_ref[:length] = split(inner)
    high_ref[length:], low_ref[length:] = split(own.T)


def send(src, dst, sems, slot, device):
    return pltpu.make_async_remote_copy(
        src_ref=src,
        dst_ref=dst,
        send_sem=sems.at[0, slot],
        recv_sem=sems.at[1, slot],
        device_id=device,
        device_id_type=pl.DeviceIdType.MESH,
    )


def greet(lev_all, lon_all):
    barrier = pltpu.get_barrier_semaphore()
    partners = []
    for axis, everyone in (("lev", lev_all), ("lon", lon_all)):
        count, me = lax.axis_size(axis), lax.axis_index(axis)
        if everyone is None:
            continue
        steps = range(1, count) if everyone else sorted({1, count - 1})
        partners += [{axis: lax.rem(me + d, count)} for d in steps if d % count]
    for device in partners:
        pl.semaphore_signal(
            barrier, inc=1, device_id=device, device_id_type=pl.DeviceIdType.MESH
        )
    pl.semaphore_wait(barrier, len(partners))


def pack_edges(cur_ref, edges_ref):
    levels, size, columns = cur_ref.shape
    lane = lax.broadcasted_iota(jnp.int32, (size, 128), 1)
    last = jnp.zeros((size, 128), jnp.float32)
    first = last
    for k in range(levels):
        tail = pltpu.roll(cur_ref[k, :, columns - 128 :], k + 1, 1)
        head = cur_ref[k, :, :128]
        head = pltpu.roll(head, k, 1) if k else head
        last = jnp.where(lane == k, tail, last)
        first = jnp.where(lane == k, head, first)
    edges_ref[0] = last
    edges_ref[1] = first


def halo_copies(edges_ref, halo_ref, sems):
    around, me = lax.axis_size("lon"), lax.axis_index("lon")
    return [
        send(edges_ref.at[0], halo_ref.at[0], sems, 0, {"lon": lax.rem(me + 1, around)}),
        send(edges_ref.at[1], halo_ref.at[1], sems, 1, {"lon": lax.rem(me + around - 1, around)}),
    ]


def local_forcing(mix_ref, cur_ref, prev_ref, pair_ref, force_ref):
    levels, size, columns = cur_ref.shape
    lane = lax.broadcasted_iota(jnp.int32, (size, columns), 1)
    for k in range(levels):
        c = cur_ref[k]
        back = jnp.where(lane == 0, 0.0, pltpu.roll(c, 1, 1))
        ahead = jnp.where(lane == columns - 1, 0.0, pltpu.roll(c, columns - 1, 1))
        p_high, p_low = split(pair_ref[k])
        chem = dot3(p_high, p_low, c * c)
        force_ref[k * size : (k + 1) * size] = (
            prev_ref[k] - chem + mix_ref[k] * (back + ahead - 2.0 * c)
        )


def add_halo(mix_ref, halo_ref, force_ref):
    levels = mix_ref.shape[0]
    size, columns = halo_ref.shape[1], force_ref.shape[1]
    lane = lax.broadcasted_iota(jnp.int32, (size, 128), 1)
    before, after = halo_ref[0], halo_ref[1]
    for k in range(levels):
        rows = slice(k * size, (k + 1) * size)
        at_head = pltpu.roll(before, 128 - k, 1) if k else before
        at_tail = pltpu.roll(after, 127 - k, 1)
        force_ref[rows, :128] += jnp.where(lane == 0, mix_ref[k] * at_head, 0.0)
        force_ref[rows, columns - 128 :] += jnp.where(lane == 127, mix_ref[k] * at_tail, 0.0)


def couple(
    links_ref, top_link, g_high, g_low, force_ref, part_ref, f_high, f_low, top_out, top_in, sides_ref,
    sems,
):
    count, me = lax.axis_size("lev"), lax.axis_index("lev")
    inner, size = part_ref.shape[0], top_out.shape[0]
    f_high[...], f_low[...] = split(force_ref[:inner])
    mul = functools.partial(jnp.dot, preferred_element_type=jnp.float32)

    def rows_of(start, stop):
        a, b = g_high[start:stop], g_low[start:stop]
        part = mul(a, f_high[...]) + (mul(b, f_high[...]) + mul(a, f_low[...]))
        part_ref[start:stop] = part
        return part

    top_out[...] = top_link * rows_of(0, size)
    sides_ref[me] = force_ref[inner:] + links_ref[inner // size - 1] * rows_of(inner - size, inner)
    up = send(top_out, top_in, sems, 0, {"lev": lax.rem(me + count - 1, count)})
    half = size * ((inner // size) // 2)

    @pl.when(me > 0)
    def _():
        up.start()

    rows_of(size, half)

    @pl.when(me < count - 1)
    def _():
        up.wait_recv()
        sides_ref[me] += top_in[...]

    copies = [
        send(sides_ref.at[me], sides_ref.at[me], sems, d, {"lev": lax.rem(me + d, count)})
        for d in range(1, count)
    ]
    for copy in copies:
        copy.start()
    rows_of(half, inner - size)

    @pl.when(me > 0)
    def _():
        up.wait_send()

    return copies


def finish(part_ref, sides_ref, high_ref, low_ref, out_ref):
    levels, size, columns = out_ref.shape
    count = sides_ref.shape[0]
    b_high, b_low = split(sides_ref[...].reshape(count * size, columns))
    mul = functools.partial(jnp.dot, preferred_element_type=jnp.float32)
    for k in range(levels):
        rows = slice(k * size, (k + 1) * size)
        a, b = high_ref[rows], low_ref[rows]
        row = mul(a, b_high) + (mul(b, b_high) + mul(a, b_low))
        out_ref[k] = row + part_ref[rows] if k < levels - 1 else row


def open_kernel(
    links_ref, mix_ref, prev_ref, pair_ref, force_ref, top_ref, edges, halo, link_out, sems
):
    levels = prev_ref.shape[0]
    count, me = lax.axis_size("lev"), lax.axis_index("lev")
    pack_edges(prev_ref, edges)
    link_out[...] = jnp.full(link_out.shape, links_ref[levels - 1], jnp.float32)
    greet(False, False)
    copies = halo_copies(edges, halo, sems)
    down = send(link_out, top_ref, sems, 2, {"lev": lax.rem(me + 1, count)})
    for copy in copies:
        copy.start()

    @pl.when(me < count - 1)
    def _():
        down.start()

    @pl.when(me == 0)
    def _():
        top_ref[...] = jnp.zeros(top_ref.shape, jnp.float32)

    local_forcing(mix_ref, prev_ref, prev_ref, pair_ref, force_ref)
    for copy in copies:
        copy.wait()
    add_halo(mix_ref, halo, force_ref)

    @pl.when(me < count - 1)
    def _():
        down.wait_send()

    @pl.when(me > 0)
    def _():
        down.wait_recv()


def gather_kernel(
    links_ref, top_ref, sent_ref, force_ref, g_high, g_low, all_ref, part_ref, sides_ref,
    f_high, f_low, top_out, top_in, sems, block_sems,
):
    count, me = lax.axis_size("lev"), lax.axis_index("lev")
    greet(True, None)
    copies = [
        send(sent_ref, all_ref.at[me], block_sems, d, {"lev": lax.rem(me + d, count)})
        for d in range(1, count)
    ]
    for copy in copies:
        copy.start()
    all_ref[me] = sent_ref[...]
    copies += couple(
        links_ref, top_ref[0:1, 0:1], g_high, g_low, force_ref, part_ref, f_high, f_low,
        top_out, top_in, sides_ref, sems,
    )
    for copy in copies:
        copy.wait()


def newton_kernel(
    links_ref, mix_ref, top_ref, part_in, sides_in, h_high, h_low, g_high, g_low, prev_ref, pair_ref,
    out_ref, var_ref, cur_ref, edges, halo, force_ref, part_ref, sides_ref, f_high, f_low,
    top_out, top_in, sums_ref, halo_sems, sems, sum_sems,
):
    levels, size, columns = prev_ref.shape
    around, place = lax.axis_size("lon"), lax.axis_index("lon")
    greet(True, True)
    finish(part_in, sides_in, h_high, h_low, cur_ref)
    pack_edges(cur_ref, edges)
    copies = halo_copies(edges, halo, halo_sems)
    for copy in copies:
        copy.start()
    local_forcing(mix_ref, cur_ref, prev_ref, pair_ref, force_ref)
    for copy in copies:
        copy.wait()
    add_halo(mix_ref, halo, force_ref)
    copies = couple(
        links_ref, top_ref[0:1, 0:1], g_high, g_low, force_ref, part_ref, f_high, f_low,
        top_out, top_in, sides_ref, sems,
    )
    for copy in copies:
        copy.wait()
    finish(part_ref, sides_ref, h_high, h_low, out_ref)
    lane = lax.broadcasted_iota(jnp.int32, (size, 128), 1)
    total = jnp.zeros((size, 128), jnp.float32)
    for k in range(levels):
        row = out_ref[k]
        total = jnp.where(lane == k, jnp.sum(row * row, axis=1, keepdims=True), total)
    sums_ref[0] = total
    copies = [
        send(sums_ref.at[0], sums_ref.at[d], sum_sems, d, {"lon": lax.rem(place + d, around)})
        for d in range(1, around)
    ]
    for copy in copies:
        copy.start()
    for copy in copies:
        copy.wait()
    total = sums_ref[place]
    for j in range(1, around):
        total = total + sums_ref[lax.rem(place - j + around, around)]
    var_ref[...] = (total / (columns * around)).T[:levels]


def call(kernel, outs, places, scratch=(), group=None):
    extra = {} if group is None else {"collective_id": group, "has_side_effects": True}
    return pl.pallas_call(
        kernel,
        out_shape=[jax.ShapeDtypeStruct(shape, dtype) for shape, dtype in outs],
        in_specs=places,
        out_specs=[VMEM] * len(outs),
        scratch_shapes=list(scratch),
        compiler_params=pltpu.CompilerParams(vmem_limit_bytes=60 * 2**20, **extra),
    )


def local(previous, loss_matrix, pair_matrix, diffusivity, mixing):
    levels, size, columns = previous.shape
    count = lax.axis_size("lev")
    around = lax.axis_size("lon")
    inner = (levels - 1) * size
    f32, bf16 = jnp.float32, jnp.bfloat16
    place = lax.axis_index("lev").astype(jnp.int32).reshape(1)
    buf, sem = pltpu.VMEM, lambda n: pltpu.SemaphoreType.DMA((2, n))
    force, top = call(
        open_kernel,
        [((levels * size, columns), f32), ((8, 128), f32)],
        [SMEM, SMEM, VMEM, VMEM],
        [buf((2, size, 128), f32), buf((2, size, 128), f32), buf((8, 128), f32), sem(3)],
        0,
    )(diffusivity, mixing, previous, pair_matrix)
    g_high, g_low, ends, sent = call(
        factor_kernel,
        [((inner, inner), bf16), ((inner, inner), bf16), ((2, inner, size), f32), ((3, size, size), f32)],
        [SMEM, VMEM, VMEM],
    )(diffusivity, top, loss_matrix)
    workspace = [buf((inner, columns), bf16)] * 2 + [buf((size, columns), f32)] * 2
    gathered, part, sides = call(
        gather_kernel,
        [((count, 3, size, size), f32), ((inner, columns), f32), ((count, size, columns), f32)],
        [SMEM] + [VMEM] * 5,
        workspace + [sem(count), sem(count)],
        1,
    )(diffusivity, top, sent, force, g_high, g_low)
    h_high, h_low = call(
        interface_kernel,
        [((levels * size, count * size), bf16)] * 2,
        [SMEM, VMEM, VMEM],
        [buf((count, count * size, size), f32)],
    )(place, gathered, ends)
    return call(
        newton_kernel,
        [((levels, size, columns), f32), ((levels, size), f32)],
        [SMEM, SMEM] + [VMEM] * 9,
        [
            buf((levels, size, columns), f32),
            buf((2, size, 128), f32),
            buf((2, size, 128), f32),
            buf((levels * size, columns), f32),
            buf((inner, columns), f32),
            buf((count, size, columns), f32),
            *workspace,
            buf((around, size, 128), f32),
            sem(2),
            sem(count),
            sem(around),
        ],
        2,
    )(diffusivity, mixing, top, part, sides, h_high, h_low, g_high, g_low, previous, pair_matrix)


def solution(mesh):
    placed = (P("lev", None, "lon"), P("lev", None, None), P("lev", None, None), P("lev"), P("lev"))
    return jax.shard_map(
        local,
        mesh=mesh,
        in_specs=placed,
        out_specs=(P("lev", None, "lon"), P("lev", None)),
        check_vma=False,
    )
```

```python
import functools

import jax
import jax.numpy as jnp
from jax import lax
from jax.experimental import pallas as pl
from jax.experimental.pallas import tpu as pltpu
from jax.sharding import PartitionSpec as P

LEAST = 1.05
MOST = 10.0
HIGHEST = lax.Precision.HIGHEST
SMEM = pl.BlockSpec(memory_space=pltpu.SMEM)
VMEM = pl.BlockSpec(memory_space=pltpu.VMEM)


def dot(a, b, dims=((1,), (0,))):
    return lax.dot_general(
        a, b, (dims, ((), ())), precision=HIGHEST, preferred_element_type=jnp.float32
    )


def dot_t(a, b):
    return dot(a, b, ((1,), (1,)))


def eye_of(size):
    rows = lax.broadcasted_iota(jnp.int32, (size, size), 0)
    cols = lax.broadcasted_iota(jnp.int32, (size, size), 1)
    return rows == cols


def invert_all(blocks, floors, steps):
    size = blocks[0].shape[0]
    unit = jnp.where(eye_of(size), 1.0, 0.0).astype(jnp.float32)
    start, worst = [], None
    for a, lo in zip(blocks, floors):
        hi = jnp.max(jnp.sum(jnp.abs(a), axis=0, keepdims=True), axis=1, keepdims=True)
        hi = jnp.clip(hi, lo, lo * spread(size))
        scale = 2.0 / (hi + lo)
        rho = (hi - lo) / (hi + lo)
        start.append((scale, a))
        worst = rho if worst is None else jnp.maximum(worst, rho)

    def grow(rho):
        square = rho * rho
        return square / (2.0 - square), 2.0 / (2.0 - square)

    rho, gain = grow(worst)
    start = [(gain * scale) * (2.0 * unit - scale * a) for scale, a in start]

    def step(carry):
        rho, *xs = carry
        rest = [unit - dot(a, x) for a, x in zip(blocks, xs)]
        rho, gain = grow(rho)
        return (rho, *[gain * (x + dot(x, r)) for x, r in zip(xs, rest)])

    if steps is None:
        return lax.while_loop(lambda carry: jnp.max(carry[0]) > 3e-8, step, (rho, *start))[1:]
    return lax.fori_loop(0, steps, lambda i, carry: step(carry), (rho, *start))[1:]


def spread(size):
    return (1.0 + MOST * size) / (0.96 * LEAST)


def enough_steps(condition):
    rho, steps = (condition - 1.0) / (condition + 1.0), -1
    while rho > 3e-8:
        rho, steps = rho * rho / (2.0 - rho * rho), steps + 1
    return steps


def plan(lo, hi, out):
    if lo >= hi:
        return 0
    mid = lo + (hi - lo) // 2
    depth = 1 + max(plan(lo, mid, out), plan(mid + 1, hi, out))
    out.setdefault(depth, []).append((lo, mid, hi))
    return depth


def dense_inverse(diag, low, floor_diag, floor_low, steps=None):
    count, size = len(diag), diag[0].shape[0]
    unit = jnp.where(eye_of(size), 1.0, 0.0).astype(jnp.float32)
    by_depth, done, thin = {}, {}, {}
    plan(0, count, by_depth)
    for depth in sorted(by_depth):
        nodes = by_depth[depth]
        schur, arms, floors, thin_arms = [], [], [], []
        for lo, mid, hi in nodes:
            s, parts = diag[mid], []
            t, thin_parts = floor_diag[mid], []
            if lo < mid:
                arm = low_right(done[lo, mid][-1], low, mid, False)
                s = s - low(mid, arm[-size:])
                parts.append(arm)
                thin_parts += [floor_low[mid] * x for x in thin[lo, mid][-1]]
                t = t - floor_low[mid] * thin_parts[-1]
            parts.append(unit)
            thin_parts.append(1.0)
            if mid + 1 < hi:
                arm = low_right(done[mid + 1, hi][0], low, mid + 1, True)
                s = s - low(mid + 1, arm[:size], True)
                parts.append(arm)
                thin_arm = [floor_low[mid + 1] * x for x in thin[mid + 1, hi][0]]
                t = t - floor_low[mid + 1] * thin_arm[0]
                thin_parts += thin_arm
            schur.append(s)
            floors.append(t)
            arms.append(jnp.concatenate(parts, axis=0) if len(parts) > 1 else parts[0])
            thin_arms.append(thin_parts)
        inverses = invert_all(schur, [0.97 * t for t in floors], steps)
        for (lo, mid, hi), v, z, thin_v, t in zip(nodes, arms, inverses, thin_arms, floors):
            thin[lo, hi] = [[a * b / t for b in thin_v] for a in thin_v]
            for a, b in ((lo, mid), (mid + 1, hi)):
                for i in range(a, b):
                    for j in range(a, b):
                        thin[lo, hi][i - lo][j - lo] += thin[a, b][i - a][j - a]
            if hi - lo == 1:
                done[lo, hi] = [z]
                continue
            w = dot(v, z)
            panels = []
            for k in range(lo, hi):
                vk = v[(k - lo) * size : (k - lo + 1) * size]
                new = w if k == mid else dot_t(w, vk)
                pieces = []
                for a, b in ((lo, mid), (mid, mid + 1), (mid + 1, hi)):
                    if a >= b:
                        continue
                    piece = new[(a - lo) * size : (b - lo) * size]
                    if a <= k < b and k != mid:
                        piece = piece + done[a, b][k - a]
                    pieces.append(piece)
                panels.append(jnp.concatenate(pieces, axis=0) if len(pieces) > 1 else pieces[0])
            done[lo, hi] = panels
    return done[0, count], thin[0, count]


def low_right(panel, low, k, plain):
    return low(k, panel, not plain, True)


def split(x):
    high = x.astype(jnp.bfloat16)
    return high, (x - high.astype(jnp.float32)).astype(jnp.bfloat16)


def dot3(a_high, a_low, b):
    b_high, b_low = split(b)
    mul = functools.partial(jnp.dot, preferred_element_type=jnp.float32)
    return mul(a_high, b_high) + (mul(a_low, b_high) + mul(a_high, b_low))


def factor_kernel(links_ref, top_ref, loss_ref, high_ref, low_ref, ends_ref, send_ref):
    levels, size = loss_ref.shape[0], loss_ref.shape[1]
    inner = levels - 1
    on_diag = eye_of(size)
    top_link, inner_link = top_ref[0:1, 0:1], jnp.full((1, 1), links_ref[inner - 1])
    links = [jnp.full((1, 1), links_ref[k]) for k in range(levels)]

    def diag_of(k):
        above = top_link if k == 0 else links[k - 1]
        return loss_ref[k] + jnp.where(on_diag, 1.0 + above + links[k], 0.0)

    def low(k, x, transposed=False, right=False):
        return links_ref[k - 1] * x

    floor_diag = [
        LEAST + links[k] + (top_link if k == 0 else links[k - 1]) for k in range(levels)
    ]
    panels, thin = dense_inverse(
        [diag_of(k) for k in range(inner)], low, floor_diag[:inner], [top_link] + links[: inner - 1]
    )
    for k, panel in enumerate(panels):
        high, rest = split(panel)
        high_ref[:, k * size : (k + 1) * size] = high
        low_ref[:, k * size : (k + 1) * size] = rest
    ends_ref[0] = top_link * panels[0]
    ends_ref[1] = inner_link * panels[-1]
    blocks = [
        (
            diag_of(inner) - inner_link * inner_link * panels[-1][-size:],
            floor_diag[inner] - inner_link * inner_link * thin[-1][-1],
        ),
        (top_link * top_link * panels[0][:size], top_link * top_link * thin[0][0]),
        (inner_link * top_link * panels[0][-size:], inner_link * top_link * thin[0][-1]),
    ]
    for k, (block, floor) in enumerate(blocks):
        send_ref[k, :size] = block
        send_ref[k, size:] = jnp.broadcast_to(floor, (8, size))


def interface(all_ref, ends_ref, high_ref, low_ref, rows_ref):
    count, size = all_ref.shape[0], all_ref.shape[3]

    def diag_of(rows, cols):
        own = [all_ref[k, 0, rows, cols] for k in range(count)]
        return [
            own[k] - all_ref[k + 1, 1, rows, cols] if k + 1 < count else own[k]
            for k in range(count)
        ]

    def low(k, x, transposed=False, right=False):
        block = all_ref[k, 2, :size]
        if right:
            return dot_t(x, block) if transposed else dot(x, block)
        return dot(block, x, ((0,), (0,))) if transposed else dot(block, x)

    thin = slice(size, size + 1), slice(0, 1)
    panels, _ = dense_inverse(
        diag_of(slice(0, size), slice(0, size)),
        low,
        diag_of(*thin),
        [all_ref[k, 2, thin[0], thin[1]] for k in range(count)],
        enough_steps(spread(size)),
    )
    for k, panel in enumerate(panels):
        rows_ref[k] = panel
    me = lax.axis_index("lev")
    own = rows_ref[me]
    above = rows_ref[jnp.maximum(me - 1, 0)]
    inner = dot_t(ends_ref[0], above) + dot_t(ends_ref[1], own)
    length = inner.shape[0]
    high_ref[:length], low_ref[:length] = split(inner)
    high_ref[length:], low_ref[length:] = split(own.T)


def send(src, dst, sems, slot, device):
    return pltpu.make_async_remote_copy(
        src_ref=src,
        dst_ref=dst,
        send_sem=sems.at[0, slot],
        recv_sem=sems.at[1, slot],
        device_id=device,
        device_id_type=pl.DeviceIdType.MESH,
    )


def greet(lev_all, lon_all):
    barrier = pltpu.get_barrier_semaphore()
    partners = []
    for axis, everyone in (("lev", lev_all), ("lon", lon_all)):
        count, me = lax.axis_size(axis), lax.axis_index(axis)
        if everyone is None:
            continue
        steps = range(1, count) if everyone else sorted({1, count - 1})
        partners += [{axis: lax.rem(me + d, count)} for d in steps if d % count]
    for device in partners:
        pl.semaphore_signal(
            barrier, inc=1, device_id=device, device_id_type=pl.DeviceIdType.MESH
        )
    pl.semaphore_wait(barrier, len(partners))


def pack_edges(cur_ref, edges_ref):
    levels, size, columns = cur_ref.shape
    lane = lax.broadcasted_iota(jnp.int32, (size, 128), 1)
    last = jnp.zeros((size, 128), jnp.float32)
    first = last
    for k in range(levels):
        tail = pltpu.roll(cur_ref[k, :, columns - 128 :], k + 1, 1)
        head = cur_ref[k, :, :128]
        head = pltpu.roll(head, k, 1) if k else head
        last = jnp.where(lane == k, tail, last)
        first = jnp.where(lane == k, head, first)
    edges_ref[0] = last
    edges_ref[1] = first


def halo_copies(edges_ref, halo_ref, sems):
    around, me = lax.axis_size("lon"), lax.axis_index("lon")
    return [
        send(edges_ref.at[0], halo_ref.at[0], sems, 0, {"lon": lax.rem(me + 1, around)}),
        send(edges_ref.at[1], halo_ref.at[1], sems, 1, {"lon": lax.rem(me + around - 1, around)}),
    ]


def local_forcing(mix_ref, cur_ref, prev_ref, pair_ref, force_ref):
    levels, size, columns = cur_ref.shape
    lane = lax.broadcasted_iota(jnp.int32, (size, columns), 1)
    for k in range(levels):
        c = cur_ref[k]
        back = jnp.where(lane == 0, 0.0, pltpu.roll(c, 1, 1))
        ahead = jnp.where(lane == columns - 1, 0.0, pltpu.roll(c, columns - 1, 1))
        p_high, p_low = split(pair_ref[k])
        chem = dot3(p_high, p_low, c * c)
        force_ref[k * size : (k + 1) * size] = (
            prev_ref[k] - chem + mix_ref[k] * (back + ahead - 2.0 * c)
        )


def add_halo(mix_ref, halo_ref, force_ref):
    levels = mix_ref.shape[0]
    size, columns = halo_ref.shape[1], force_ref.shape[1]
    lane = lax.broadcasted_iota(jnp.int32, (size, 128), 1)
    before, after = halo_ref[0], halo_ref[1]
    for k in range(levels):
        rows = slice(k * size, (k + 1) * size)
        at_head = pltpu.roll(before, 128 - k, 1) if k else before
        at_tail = pltpu.roll(after, 127 - k, 1)
        force_ref[rows, :128] += jnp.where(lane == 0, mix_ref[k] * at_head, 0.0)
        force_ref[rows, columns - 128 :] += jnp.where(lane == 127, mix_ref[k] * at_tail, 0.0)


def couple(
    links_ref, top_link, g_high, g_low, force_ref, part_ref, f_high, f_low, top_out, top_in, sides_ref,
    sems,
):
    count, me = lax.axis_size("lev"), lax.axis_index("lev")
    inner, size = part_ref.shape[0], top_out.shape[0]
    f_high[...], f_low[...] = split(force_ref[:inner])
    mul = functools.partial(jnp.dot, preferred_element_type=jnp.float32)

    def rows_of(start, stop):
        a, b = g_high[start:stop], g_low[start:stop]
        part = mul(a, f_high[...]) + (mul(b, f_high[...]) + mul(a, f_low[...]))
        part_ref[start:stop] = part
        return part

    top_out[...] = top_link * rows_of(0, size)
    sides_ref[me] = force_ref[inner:] + links_ref[inner // size - 1] * rows_of(inner - size, inner)
    up = send(top_out, top_in, sems, 0, {"lev": lax.rem(me + count - 1, count)})
    half = size * ((inner // size) // 2)

    @pl.when(me > 0)
    def _():
        up.start()

    rows_of(size, half)

    @pl.when(me < count - 1)
    def _():
        up.wait_recv()
        sides_ref[me] += top_in[...]

    copies = [
        send(sides_ref.at[me], sides_ref.at[me], sems, d, {"lev": lax.rem(me + d, count)})
        for d in range(1, count)
    ]
    for copy in copies:
        copy.start()
    rows_of(half, inner - size)

    @pl.when(me > 0)
    def _():
        up.wait_send()

    return copies


def finish(part_ref, sides_ref, high_ref, low_ref, out_ref):
    levels, size, columns = out_ref.shape
    count = sides_ref.shape[0]
    b_high, b_low = split(sides_ref[...].reshape(count * size, columns))
    mul = functools.partial(jnp.dot, preferred_element_type=jnp.float32)
    for k in range(levels):
        rows = slice(k * size, (k + 1) * size)
        a, b = high_ref[rows], low_ref[rows]
        row = mul(a, b_high) + (mul(b, b_high) + mul(a, b_low))
        out_ref[k] = row + part_ref[rows] if k < levels - 1 else row


def open_kernel(
    links_ref, mix_ref, prev_ref, pair_ref, force_ref, top_ref, edges, halo, link_out, sems
):
    levels = prev_ref.shape[0]
    count, me = lax.axis_size("lev"), lax.axis_index("lev")
    pack_edges(prev_ref, edges)
    link_out[...] = jnp.full(link_out.shape, links_ref[levels - 1], jnp.float32)
    greet(False, False)
    copies = halo_copies(edges, halo, sems)
    down = send(link_out, top_ref, sems, 2, {"lev": lax.rem(me + 1, count)})
    for copy in copies:
        copy.start()

    @pl.when(me < count - 1)
    def _():
        down.start()

    @pl.when(me == 0)
    def _():
        top_ref[...] = jnp.zeros(top_ref.shape, jnp.float32)

    local_forcing(mix_ref, prev_ref, prev_ref, pair_ref, force_ref)
    for copy in copies:
        copy.wait()
    add_halo(mix_ref, halo, force_ref)

    @pl.when(me < count - 1)
    def _():
        down.wait_send()

    @pl.when(me > 0)
    def _():
        down.wait_recv()


def newton_kernel(
    links_ref, mix_ref, top_ref, sent_ref, ends_ref, first_force, g_high, g_low, prev_ref, pair_ref,
    out_ref, var_ref, all_ref, rows_ref, h_high, h_low, cur_ref, edges, halo, force_ref, part_ref,
    first_sides, sides_ref, f_high, f_low, first_out, first_in, top_out, top_in, sums_ref,
    block_sems, first_sems, halo_sems, sems, sum_sems,
):
    levels, size, columns = prev_ref.shape
    count, me = lax.axis_size("lev"), lax.axis_index("lev")
    around, place = lax.axis_size("lon"), lax.axis_index("lon")
    greet(True, True)
    blocks = [
        send(sent_ref, all_ref.at[me], block_sems, d, {"lev": lax.rem(me + d, count)})
        for d in range(1, count)
    ]
    for copy in blocks:
        copy.start()
    all_ref[me] = sent_ref[...]
    copies = couple(
        links_ref, top_ref[0:1, 0:1], g_high, g_low, first_force, part_ref, f_high, f_low,
        first_out, first_in, first_sides, first_sems,
    )
    for copy in blocks:
        copy.wait()
    interface(all_ref, ends_ref, h_high, h_low, rows_ref)
    for copy in copies:
        copy.wait()
    finish(part_ref, first_sides, h_high, h_low, cur_ref)
    pack_edges(cur_ref, edges)
    copies = halo_copies(edges, halo, halo_sems)
    for copy in copies:
        copy.start()
    local_forcing(mix_ref, cur_ref, prev_ref, pair_ref, force_ref)
    for copy in copies:
        copy.wait()
    add_halo(mix_ref, halo, force_ref)
    copies = couple(
        links_ref, top_ref[0:1, 0:1], g_high, g_low, force_ref, part_ref, f_high, f_low,
        top_out, top_in, sides_ref, sems,
    )
    for copy in copies:
        copy.wait()
    finish(part_ref, sides_ref, h_high, h_low, out_ref)
    lane = lax.broadcasted_iota(jnp.int32, (size, 128), 1)
    total = jnp.zeros((size, 128), jnp.float32)
    for k in range(levels):
        row = out_ref[k]
        total = jnp.where(lane == k, jnp.sum(row * row, axis=1, keepdims=True), total)
    sums_ref[0] = total
    copies = [
        send(sums_ref.at[0], sums_ref.at[d], sum_sems, d, {"lon": lax.rem(place + d, around)})
        for d in range(1, around)
    ]
    for copy in copies:
        copy.start()
    for copy in copies:
        copy.wait()
    total = sums_ref[place]
    for j in range(1, around):
        total = total + sums_ref[lax.rem(place - j + around, around)]
    var_ref[...] = (total / (columns * around)).T[:levels]


def call(kernel, outs, places, scratch=(), group=None):
    extra = {} if group is None else {"collective_id": group, "has_side_effects": True}
    return pl.pallas_call(
        kernel,
        out_shape=[jax.ShapeDtypeStruct(shape, dtype) for shape, dtype in outs],
        in_specs=places,
        out_specs=[VMEM] * len(outs),
        scratch_shapes=list(scratch),
        compiler_params=pltpu.CompilerParams(vmem_limit_bytes=60 * 2**20, **extra),
    )


def local(previous, loss_matrix, pair_matrix, diffusivity, mixing):
    levels, size, columns = previous.shape
    count = lax.axis_size("lev")
    around = lax.axis_size("lon")
    inner = (levels - 1) * size
    f32, bf16 = jnp.float32, jnp.bfloat16
    buf, sem = pltpu.VMEM, lambda n: pltpu.SemaphoreType.DMA((2, n))
    force, top = call(
        open_kernel,
        [((levels * size, columns), f32), ((8, 128), f32)],
        [SMEM, SMEM, VMEM, VMEM],
        [buf((2, size, 128), f32), buf((2, size, 128), f32), buf((8, 128), f32), sem(3)],
        0,
    )(diffusivity, mixing, previous, pair_matrix)
    g_high, g_low, ends, sent = call(
        factor_kernel,
        [((inner, inner), bf16), ((inner, inner), bf16), ((2, inner, size), f32), ((3, size + 8, size), f32)],
        [SMEM, VMEM, VMEM],
    )(diffusivity, top, loss_matrix)
    return call(
        newton_kernel,
        [((levels, size, columns), f32), ((levels, size), f32)],
        [SMEM, SMEM] + [VMEM] * 8,
        [
            buf((count, 3, size + 8, size), f32),
            buf((count, count * size, size), f32),
            buf((levels * size, count * size), bf16),
            buf((levels * size, count * size), bf16),
            buf((levels, size, columns), f32),
            buf((2, size, 128), f32),
            buf((2, size, 128), f32),
            buf((levels * size, columns), f32),
            buf((inner, columns), f32),
            buf((count, size, columns), f32),
            buf((count, size, columns), f32),
            buf((inner, columns), bf16),
            buf((inner, columns), bf16),
            buf((size, columns), f32),
            buf((size, columns), f32),
            buf((size, columns), f32),
            buf((size, columns), f32),
            buf((around, size, 128), f32),
            sem(count),
            sem(count),
            sem(2),
            sem(count),
            sem(around),
        ],
        1,
    )(diffusivity, mixing, top, sent, ends, force, g_high, g_low, previous, pair_matrix)


def solution(mesh):
    placed = (P("lev", None, "lon"), P("lev", None, None), P("lev", None, None), P("lev"), P("lev"))
    return jax.shard_map(
        local,
        mesh=mesh,
        in_specs=placed,
        out_specs=(P("lev", None, "lon"), P("lev", None)),
        check_vma=False,
    )
```

```python
import functools

import jax
import jax.numpy as jnp
from jax import lax
from jax.experimental import pallas as pl
from jax.experimental.pallas import tpu as pltpu
from jax.sharding import PartitionSpec as P

LEAST = 1.05
MOST = 10.0
HIGHEST = lax.Precision.HIGHEST
SMEM = pl.BlockSpec(memory_space=pltpu.SMEM)
VMEM = pl.BlockSpec(memory_space=pltpu.VMEM)


def dot(a, b, dims=((1,), (0,))):
    return lax.dot_general(
        a, b, (dims, ((), ())), precision=HIGHEST, preferred_element_type=jnp.float32
    )


def dot_t(a, b):
    return dot(a, b, ((1,), (1,)))


def eye_of(size):
    rows = lax.broadcasted_iota(jnp.int32, (size, size), 0)
    cols = lax.broadcasted_iota(jnp.int32, (size, size), 1)
    return rows == cols


def invert_all(blocks, floors, steps):
    size = blocks[0].shape[0]
    unit = jnp.where(eye_of(size), 1.0, 0.0).astype(jnp.float32)
    start, worst = [], None
    for a, lo in zip(blocks, floors):
        hi = jnp.max(jnp.sum(jnp.abs(a), axis=0, keepdims=True), axis=1, keepdims=True)
        hi = jnp.clip(hi, lo, lo * spread(size))
        scale = 2.0 / (hi + lo)
        rho = (hi - lo) / (hi + lo)
        start.append((scale, a))
        worst = rho if worst is None else jnp.maximum(worst, rho)

    def grow(rho):
        square = rho * rho
        return square / (2.0 - square), 2.0 / (2.0 - square)

    rho, gain = grow(worst)
    start = [(gain * scale) * (2.0 * unit - scale * a) for scale, a in start]

    def step(carry):
        rho, *xs = carry
        rest = [unit - dot(a, x) for a, x in zip(blocks, xs)]
        rho, gain = grow(rho)
        return (rho, *[gain * (x + dot(x, r)) for x, r in zip(xs, rest)])

    if steps is None:
        return lax.while_loop(lambda carry: jnp.max(carry[0]) > 3e-8, step, (rho, *start))[1:]
    return lax.fori_loop(0, steps, lambda i, carry: step(carry), (rho, *start))[1:]


def spread(size):
    return (1.0 + MOST * size) / (0.96 * LEAST)


def enough_steps(condition):
    rho, steps = (condition - 1.0) / (condition + 1.0), -1
    while rho > 3e-8:
        rho, steps = rho * rho / (2.0 - rho * rho), steps + 1
    return steps


def plan(lo, hi, out):
    if lo >= hi:
        return 0
    mid = lo + (hi - lo) // 2
    depth = 1 + max(plan(lo, mid, out), plan(mid + 1, hi, out))
    out.setdefault(depth, []).append((lo, mid, hi))
    return depth


def dense_inverse(diag, low, floor_diag, floor_low, steps=None):
    count, size = len(diag), diag[0].shape[0]
    unit = jnp.where(eye_of(size), 1.0, 0.0).astype(jnp.float32)
    by_depth, done, thin = {}, {}, {}
    plan(0, count, by_depth)
    for depth in sorted(by_depth):
        nodes = by_depth[depth]
        schur, arms, floors, thin_arms = [], [], [], []
        for lo, mid, hi in nodes:
            s, parts = diag[mid], []
            t, thin_parts = floor_diag[mid], []
            if lo < mid:
                arm = low_right(done[lo, mid][-1], low, mid, False)
                s = s - low(mid, arm[-size:])
                parts.append(arm)
                thin_parts += [floor_low[mid] * x for x in thin[lo, mid][-1]]
                t = t - floor_low[mid] * thin_parts[-1]
            parts.append(unit)
            thin_parts.append(1.0)
            if mid + 1 < hi:
                arm = low_right(done[mid + 1, hi][0], low, mid + 1, True)
                s = s - low(mid + 1, arm[:size], True)
                parts.append(arm)
                thin_arm = [floor_low[mid + 1] * x for x in thin[mid + 1, hi][0]]
                t = t - floor_low[mid + 1] * thin_arm[0]
                thin_parts += thin_arm
            schur.append(s)
            floors.append(t)
            arms.append(jnp.concatenate(parts, axis=0) if len(parts) > 1 else parts[0])
            thin_arms.append(thin_parts)
        inverses = invert_all(schur, [0.97 * t for t in floors], steps)
        for (lo, mid, hi), v, z, thin_v, t in zip(nodes, arms, inverses, thin_arms, floors):
            thin[lo, hi] = [[a * b / t for b in thin_v] for a in thin_v]
            for a, b in ((lo, mid), (mid + 1, hi)):
                for i in range(a, b):
                    for j in range(a, b):
                        thin[lo, hi][i - lo][j - lo] += thin[a, b][i - a][j - a]
            if hi - lo == 1:
                done[lo, hi] = [z]
                continue
            w = dot(v, z)
            panels = []
            for k in range(lo, hi):
                vk = v[(k - lo) * size : (k - lo + 1) * size]
                new = w if k == mid else dot_t(w, vk)
                pieces = []
                for a, b in ((lo, mid), (mid, mid + 1), (mid + 1, hi)):
                    if a >= b:
                        continue
                    piece = new[(a - lo) * size : (b - lo) * size]
                    if a <= k < b and k != mid:
                        piece = piece + done[a, b][k - a]
                    pieces.append(piece)
                panels.append(jnp.concatenate(pieces, axis=0) if len(pieces) > 1 else pieces[0])
            done[lo, hi] = panels
    return done[0, count], thin[0, count]


def low_right(panel, low, k, plain):
    return low(k, panel, not plain, True)


def split(x):
    high = x.astype(jnp.bfloat16)
    return high, (x - high.astype(jnp.float32)).astype(jnp.bfloat16)


def dot3(a_high, a_low, b):
    b_high, b_low = split(b)
    mul = functools.partial(jnp.dot, preferred_element_type=jnp.float32)
    return mul(a_high, b_high) + (mul(a_low, b_high) + mul(a_high, b_low))


def factor_kernel(links_ref, top_ref, loss_ref, high_ref, low_ref, ends_ref, send_ref):
    levels, size = loss_ref.shape[0], loss_ref.shape[1]
    inner = levels - 1
    on_diag = eye_of(size)
    top_link, inner_link = top_ref[0:1, 0:1], jnp.full((1, 1), links_ref[inner - 1])
    links = [jnp.full((1, 1), links_ref[k]) for k in range(levels)]

    def diag_of(k):
        above = top_link if k == 0 else links[k - 1]
        return loss_ref[k] + jnp.where(on_diag, 1.0 + above + links[k], 0.0)

    def low(k, x, transposed=False, right=False):
        return links_ref[k - 1] * x

    floor_diag = [
        LEAST + links[k] + (top_link if k == 0 else links[k - 1]) for k in range(levels)
    ]
    panels, thin = dense_inverse(
        [diag_of(k) for k in range(inner)], low, floor_diag[:inner], [top_link] + links[: inner - 1]
    )
    for k, panel in enumerate(panels):
        high, rest = split(panel)
        high_ref[:, k * size : (k + 1) * size] = high
        low_ref[:, k * size : (k + 1) * size] = rest
    ends_ref[0] = top_link * panels[0]
    ends_ref[1] = inner_link * panels[-1]
    blocks = [
        (
            diag_of(inner) - inner_link * inner_link * panels[-1][-size:],
            floor_diag[inner] - inner_link * inner_link * thin[-1][-1],
        ),
        (top_link * top_link * panels[0][:size], top_link * top_link * thin[0][0]),
        (inner_link * top_link * panels[0][-size:], inner_link * top_link * thin[0][-1]),
    ]
    for k, (block, floor) in enumerate(blocks):
        send_ref[k, :size] = block
        send_ref[k, size:] = jnp.broadcast_to(floor, (8, size))


def interface(all_ref, ends_ref, high_ref, low_ref, rows_ref):
    count, size = all_ref.shape[0], all_ref.shape[3]

    def diag_of(rows, cols):
        own = [all_ref[k, 0, rows, cols] for k in range(count)]
        return [
            own[k] - all_ref[k + 1, 1, rows, cols] if k + 1 < count else own[k]
            for k in range(count)
        ]

    def low(k, x, transposed=False, right=False):
        block = all_ref[k, 2, :size]
        if right:
            return dot_t(x, block) if transposed else dot(x, block)
        return dot(block, x, ((0,), (0,))) if transposed else dot(block, x)

    thin = slice(size, size + 1), slice(0, 1)
    panels, _ = dense_inverse(
        diag_of(slice(0, size), slice(0, size)),
        low,
        diag_of(*thin),
        [all_ref[k, 2, thin[0], thin[1]] for k in range(count)],
        enough_steps(spread(size)),
    )
    for k, panel in enumerate(panels):
        rows_ref[k] = panel
    me = lax.axis_index("lev")
    own = rows_ref[me]
    above = rows_ref[jnp.maximum(me - 1, 0)]
    inner = dot_t(ends_ref[0], above) + dot_t(ends_ref[1], own)
    length = inner.shape[0]
    high_ref[:length], low_ref[:length] = split(inner)
    high_ref[length:], low_ref[length:] = split(own.T)


def send(src, dst, sems, slot, device):
    return pltpu.make_async_remote_copy(
        src_ref=src,
        dst_ref=dst,
        send_sem=sems.at[0, slot],
        recv_sem=sems.at[1, slot],
        device_id=device,
        device_id_type=pl.DeviceIdType.MESH,
    )


def greet(lev_all, lon_all):
    barrier = pltpu.get_barrier_semaphore()
    partners = []
    for axis, everyone in (("lev", lev_all), ("lon", lon_all)):
        count, me = lax.axis_size(axis), lax.axis_index(axis)
        if everyone is None:
            continue
        steps = range(1, count) if everyone else sorted({1, count - 1})
        partners += [{axis: lax.rem(me + d, count)} for d in steps if d % count]
    for device in partners:
        pl.semaphore_signal(
            barrier, inc=1, device_id=device, device_id_type=pl.DeviceIdType.MESH
        )
    pl.semaphore_wait(barrier, len(partners))


def pack_edges(cur_ref, edges_ref):
    levels, size, columns = cur_ref.shape
    lane = lax.broadcasted_iota(jnp.int32, (size, 128), 1)
    last = jnp.zeros((size, 128), jnp.float32)
    first = last
    for k in range(levels):
        tail = pltpu.roll(cur_ref[k, :, columns - 128 :], k + 1, 1)
        head = cur_ref[k, :, :128]
        head = pltpu.roll(head, k, 1) if k else head
        last = jnp.where(lane == k, tail, last)
        first = jnp.where(lane == k, head, first)
    edges_ref[0] = last
    edges_ref[1] = first


def halo_copies(edges_ref, halo_ref, sems):
    around, me = lax.axis_size("lon"), lax.axis_index("lon")
    return [
        send(edges_ref.at[0], halo_ref.at[0], sems, 0, {"lon": lax.rem(me + 1, around)}),
        send(edges_ref.at[1], halo_ref.at[1], sems, 1, {"lon": lax.rem(me + around - 1, around)}),
    ]


def local_forcing(mix_ref, cur_ref, prev_ref, pair_ref, force_ref):
    levels, size, columns = cur_ref.shape
    lane = lax.broadcasted_iota(jnp.int32, (size, columns), 1)
    for k in range(levels):
        c = cur_ref[k]
        back = jnp.where(lane == 0, 0.0, pltpu.roll(c, 1, 1))
        ahead = jnp.where(lane == columns - 1, 0.0, pltpu.roll(c, columns - 1, 1))
        p_high, p_low = split(pair_ref[k])
        chem = dot3(p_high, p_low, c * c)
        force_ref[k * size : (k + 1) * size] = (
            prev_ref[k] - chem + mix_ref[k] * (back + ahead - 2.0 * c)
        )


def add_halo(mix_ref, halo_ref, force_ref):
    levels = mix_ref.shape[0]
    size, columns = halo_ref.shape[1], force_ref.shape[1]
    lane = lax.broadcasted_iota(jnp.int32, (size, 128), 1)
    before, after = halo_ref[0], halo_ref[1]
    for k in range(levels):
        rows = slice(k * size, (k + 1) * size)
        at_head = pltpu.roll(before, 128 - k, 1) if k else before
        at_tail = pltpu.roll(after, 127 - k, 1)
        force_ref[rows, :128] += jnp.where(lane == 0, mix_ref[k] * at_head, 0.0)
        force_ref[rows, columns - 128 :] += jnp.where(lane == 127, mix_ref[k] * at_tail, 0.0)


def couple(
    links_ref, top_link, g_high, g_low, force_ref, part_ref, f_high, f_low, top_out, top_in, sides_ref,
    sems,
):
    count, me = lax.axis_size("lev"), lax.axis_index("lev")
    inner, size = part_ref.shape[0], top_out.shape[0]
    f_high[...], f_low[...] = split(force_ref[:inner])
    mul = functools.partial(jnp.dot, preferred_element_type=jnp.float32)

    def rows_of(start, stop):
        a, b = g_high[start:stop], g_low[start:stop]
        part = mul(a, f_high[...]) + (mul(b, f_high[...]) + mul(a, f_low[...]))
        part_ref[start:stop] = part
        return part

    top_out[...] = top_link * rows_of(0, size)
    sides_ref[me] = force_ref[inner:] + links_ref[inner // size - 1] * rows_of(inner - size, inner)
    up = send(top_out, top_in, sems, 0, {"lev": lax.rem(me + count - 1, count)})
    half = size * ((inner // size) // 2)

    @pl.when(me > 0)
    def _():
        up.start()

    rows_of(size, half)

    @pl.when(me < count - 1)
    def _():
        up.wait_recv()
        sides_ref[me] += top_in[...]

    copies = [
        send(sides_ref.at[me], sides_ref.at[me], sems, d, {"lev": lax.rem(me + d, count)})
        for d in range(1, count)
    ]
    for copy in copies:
        copy.start()
    rows_of(half, inner - size)

    @pl.when(me > 0)
    def _():
        up.wait_send()

    return copies


def finish(part_ref, sides_ref, high_ref, low_ref, out_ref):
    levels, size, columns = out_ref.shape
    count = sides_ref.shape[0]
    b_high, b_low = split(sides_ref[...].reshape(count * size, columns))
    mul = functools.partial(jnp.dot, preferred_element_type=jnp.float32)
    for k in range(levels):
        rows = slice(k * size, (k + 1) * size)
        a, b = high_ref[rows], low_ref[rows]
        row = mul(a, b_high) + (mul(b, b_high) + mul(a, b_low))
        out_ref[k] = row + part_ref[rows] if k < levels - 1 else row


def open_kernel(
    links_ref, mix_ref, prev_ref, pair_ref, force_ref, top_ref, edges, halo, link_out, sems
):
    levels = prev_ref.shape[0]
    count, me = lax.axis_size("lev"), lax.axis_index("lev")
    pack_edges(prev_ref, edges)
    link_out[...] = jnp.full(link_out.shape, links_ref[levels - 1], jnp.float32)
    greet(False, False)
    copies = halo_copies(edges, halo, sems)
    down = send(link_out, top_ref, sems, 2, {"lev": lax.rem(me + 1, count)})
    for copy in copies:
        copy.start()

    @pl.when(me < count - 1)
    def _():
        down.start()

    @pl.when(me == 0)
    def _():
        top_ref[...] = jnp.zeros(top_ref.shape, jnp.float32)

    local_forcing(mix_ref, prev_ref, prev_ref, pair_ref, force_ref)
    for copy in copies:
        copy.wait()
    add_halo(mix_ref, halo, force_ref)

    @pl.when(me < count - 1)
    def _():
        down.wait_send()

    @pl.when(me > 0)
    def _():
        down.wait_recv()


def newton_kernel(
    links_ref, mix_ref, top_ref, sent_ref, ends_ref, first_force, g_high, g_low, prev_ref, pair_ref,
    out_ref, var_ref, all_ref, rows_ref, h_high, h_low, cur_ref, edges, halo, force_ref, part_ref,
    first_sides, sides_ref, f_high, f_low, first_out, first_in, top_out, top_in, sums_ref,
    block_sems, first_sems, halo_sems, sems, sum_sems,
):
    levels, size, columns = prev_ref.shape
    count, me = lax.axis_size("lev"), lax.axis_index("lev")
    around, place = lax.axis_size("lon"), lax.axis_index("lon")
    greet(True, True)
    blocks = [
        send(sent_ref, all_ref.at[me], block_sems, d, {"lev": lax.rem(me + d, count)})
        for d in range(1, count)
    ]
    for copy in blocks:
        copy.start()
    all_ref[me] = sent_ref[...]
    copies = couple(
        links_ref, top_ref[0:1, 0:1], g_high, g_low, first_force, part_ref, f_high, f_low,
        first_out, first_in, first_sides, first_sems,
    )
    for copy in blocks:
        copy.wait()
    interface(all_ref, ends_ref, h_high, h_low, rows_ref)
    for copy in copies:
        copy.wait()
    finish(part_ref, first_sides, h_high, h_low, cur_ref)
    pack_edges(cur_ref, edges)
    copies = halo_copies(edges, halo, halo_sems)
    for copy in copies:
        copy.start()
    local_forcing(mix_ref, cur_ref, prev_ref, pair_ref, force_ref)
    for copy in copies:
        copy.wait()
    add_halo(mix_ref, halo, force_ref)
    copies = couple(
        links_ref, top_ref[0:1, 0:1], g_high, g_low, force_ref, part_ref, f_high, f_low,
        top_out, top_in, sides_ref, sems,
    )
    for copy in copies:
        copy.wait()
    finish(part_ref, sides_ref, h_high, h_low, out_ref)
    lane = lax.broadcasted_iota(jnp.int32, (size, 128), 1)
    total = jnp.zeros((size, 128), jnp.float32)
    for k in range(levels):
        row = out_ref[k]
        total = jnp.where(lane == k, jnp.sum(row * row, axis=1, keepdims=True), total)
    sums_ref[0] = total.T[: sums_ref.shape[1]]
    copies = [
        send(sums_ref.at[0], sums_ref.at[d], sum_sems, d, {"lon": lax.rem(place + d, around)})
        for d in range(1, around)
    ]
    for copy in copies:
        copy.start()
    for copy in copies:
        copy.wait()
    total = sums_ref[place]
    for j in range(1, around):
        total = total + sums_ref[lax.rem(place - j + around, around)]
    var_ref[...] = (total / (columns * around))[:levels]


def call(kernel, outs, places, scratch=(), group=None):
    extra = {} if group is None else {"collective_id": group, "has_side_effects": True}
    return pl.pallas_call(
        kernel,
        out_shape=[jax.ShapeDtypeStruct(shape, dtype) for shape, dtype in outs],
        in_specs=places,
        out_specs=[VMEM] * len(outs),
        scratch_shapes=list(scratch),
        compiler_params=pltpu.CompilerParams(vmem_limit_bytes=60 * 2**20, **extra),
    )


def local(previous, loss_matrix, pair_matrix, diffusivity, mixing):
    levels, size, columns = previous.shape
    count = lax.axis_size("lev")
    around = lax.axis_size("lon")
    inner = (levels - 1) * size
    f32, bf16 = jnp.float32, jnp.bfloat16
    buf, sem = pltpu.VMEM, lambda n: pltpu.SemaphoreType.DMA((2, n))
    force, top = call(
        open_kernel,
        [((levels * size, columns), f32), ((8, 128), f32)],
        [SMEM, SMEM, VMEM, VMEM],
        [buf((2, size, 128), f32), buf((2, size, 128), f32), buf((8, 128), f32), sem(3)],
        0,
    )(diffusivity, mixing, previous, pair_matrix)
    g_high, g_low, ends, sent = call(
        factor_kernel,
        [((inner, inner), bf16), ((inner, inner), bf16), ((2, inner, size), f32), ((3, size + 8, size), f32)],
        [SMEM, VMEM, VMEM],
    )(diffusivity, top, loss_matrix)
    return call(
        newton_kernel,
        [((levels, size, columns), f32), ((levels, size), f32)],
        [SMEM, SMEM] + [VMEM] * 8,
        [
            buf((count, 3, size + 8, size), f32),
            buf((count, count * size, size), f32),
            buf((levels * size, count * size), bf16),
            buf((levels * size, count * size), bf16),
            buf((levels, size, columns), f32),
            buf((2, size, 128), f32),
            buf((2, size, 128), f32),
            buf((levels * size, columns), f32),
            buf((inner, columns), f32),
            buf((count, size, columns), f32),
            buf((count, size, columns), f32),
            buf((inner, columns), bf16),
            buf((inner, columns), bf16),
            buf((size, columns), f32),
            buf((size, columns), f32),
            buf((size, columns), f32),
            buf((size, columns), f32),
            buf((around, -(-levels // 8) * 8, size), f32),
            sem(count),
            sem(count),
            sem(2),
            sem(count),
            sem(around),
        ],
        1,
    )(diffusivity, mixing, top, sent, ends, force, g_high, g_low, previous, pair_matrix)


def solution(mesh):
    placed = (P("lev", None, "lon"), P("lev", None, None), P("lev", None, None), P("lev"), P("lev"))
    return jax.shard_map(
        local,
        mesh=mesh,
        in_specs=placed,
        out_specs=(P("lev", None, "lon"), P("lev", None)),
        check_vma=False,
    )
```

```python
import functools

import jax
import jax.numpy as jnp
from jax import lax
from jax.experimental import pallas as pl
from jax.experimental.pallas import tpu as pltpu
from jax.sharding import PartitionSpec as P

LEAST = 1.05
MOST = 10.0
HIGHEST = lax.Precision.HIGHEST
SMEM = pl.BlockSpec(memory_space=pltpu.SMEM)
VMEM = pl.BlockSpec(memory_space=pltpu.VMEM)


def dot(a, b, dims=((1,), (0,))):
    return lax.dot_general(
        a, b, (dims, ((), ())), precision=HIGHEST, preferred_element_type=jnp.float32
    )


def dot_t(a, b):
    return dot(a, b, ((1,), (1,)))


def eye_of(size):
    rows = lax.broadcasted_iota(jnp.int32, (size, size), 0)
    cols = lax.broadcasted_iota(jnp.int32, (size, size), 1)
    return rows == cols


def invert_all(blocks, floors, steps):
    size = blocks[0].shape[0]
    unit = jnp.where(eye_of(size), 1.0, 0.0).astype(jnp.float32)
    start, worst = [], None
    for a, lo in zip(blocks, floors):
        hi = jnp.max(jnp.sum(jnp.abs(a), axis=0, keepdims=True), axis=1, keepdims=True)
        hi = jnp.clip(hi, lo, lo * spread(size))
        scale = 2.0 / (hi + lo)
        rho = (hi - lo) / (hi + lo)
        start.append((scale, a))
        worst = rho if worst is None else jnp.maximum(worst, rho)

    def grow(rho):
        square = rho * rho
        return square / (2.0 - square), 2.0 / (2.0 - square)

    rho, gain = grow(worst)
    start = [(gain * scale) * (2.0 * unit - scale * a) for scale, a in start]

    def step(carry):
        rho, *xs = carry
        rest = [unit - dot(a, x) for a, x in zip(blocks, xs)]
        rho, gain = grow(rho)
        return (rho, *[gain * (x + dot(x, r)) for x, r in zip(xs, rest)])

    if steps is None:
        return lax.while_loop(lambda carry: jnp.max(carry[0]) > 3e-8, step, (rho, *start))[1:]
    return lax.fori_loop(0, steps, lambda i, carry: step(carry), (rho, *start))[1:]


def spread(size):
    return (1.0 + MOST * size) / (0.96 * LEAST)


def enough_steps(condition):
    rho, steps = (condition - 1.0) / (condition + 1.0), -1
    while rho > 3e-8:
        rho, steps = rho * rho / (2.0 - rho * rho), steps + 1
    return steps


def plan(lo, hi, out):
    if lo >= hi:
        return 0
    mid = lo + (hi - lo) // 2
    depth = 1 + max(plan(lo, mid, out), plan(mid + 1, hi, out))
    out.setdefault(depth, []).append((lo, mid, hi))
    return depth


def dense_inverse(diag, low, floor_diag, floor_low, steps=None):
    count, size = len(diag), diag[0].shape[0]
    unit = jnp.where(eye_of(size), 1.0, 0.0).astype(jnp.float32)
    by_depth, done, thin = {}, {}, {}
    plan(0, count, by_depth)
    for depth in sorted(by_depth):
        nodes = by_depth[depth]
        schur, arms, floors, thin_arms = [], [], [], []
        for lo, mid, hi in nodes:
            s, parts = diag[mid], []
            t, thin_parts = floor_diag[mid], []
            if lo < mid:
                arm = low_right(done[lo, mid][-1], low, mid, False)
                s = s - low(mid, arm[-size:])
                parts.append(arm)
                thin_parts += [floor_low[mid] * x for x in thin[lo, mid][-1]]
                t = t - floor_low[mid] * thin_parts[-1]
            parts.append(unit)
            thin_parts.append(1.0)
            if mid + 1 < hi:
                arm = low_right(done[mid + 1, hi][0], low, mid + 1, True)
                s = s - low(mid + 1, arm[:size], True)
                parts.append(arm)
                thin_arm = [floor_low[mid + 1] * x for x in thin[mid + 1, hi][0]]
                t = t - floor_low[mid + 1] * thin_arm[0]
                thin_parts += thin_arm
            schur.append(s)
            floors.append(t)
            arms.append(jnp.concatenate(parts, axis=0) if len(parts) > 1 else parts[0])
            thin_arms.append(thin_parts)
        inverses = invert_all(schur, [0.97 * t for t in floors], steps)
        for (lo, mid, hi), v, z, thin_v, t in zip(nodes, arms, inverses, thin_arms, floors):
            thin[lo, hi] = [[a * b / t for b in thin_v] for a in thin_v]
            for a, b in ((lo, mid), (mid + 1, hi)):
                for i in range(a, b):
                    for j in range(a, b):
                        thin[lo, hi][i - lo][j - lo] += thin[a, b][i - a][j - a]
            if hi - lo == 1:
                done[lo, hi] = [z]
                continue
            w = dot(v, z)
            panels = []
            for k in range(lo, hi):
                vk = v[(k - lo) * size : (k - lo + 1) * size]
                new = w if k == mid else dot_t(w, vk)
                pieces = []
                for a, b in ((lo, mid), (mid, mid + 1), (mid + 1, hi)):
                    if a >= b:
                        continue
                    piece = new[(a - lo) * size : (b - lo) * size]
                    if a <= k < b and k != mid:
                        piece = piece + done[a, b][k - a]
                    pieces.append(piece)
                panels.append(jnp.concatenate(pieces, axis=0) if len(pieces) > 1 else pieces[0])
            done[lo, hi] = panels
    return done[0, count], thin[0, count]


def low_right(panel, low, k, plain):
    return low(k, panel, not plain, True)


def split(x):
    high = x.astype(jnp.bfloat16)
    return high, (x - high.astype(jnp.float32)).astype(jnp.bfloat16)


def dot3(a_high, a_low, b):
    b_high, b_low = split(b)
    mul = functools.partial(jnp.dot, preferred_element_type=jnp.float32)
    return mul(a_high, b_high) + (mul(a_low, b_high) + mul(a_high, b_low))


def factor_kernel(links_ref, top_ref, loss_ref, high_ref, low_ref, ends_ref, send_ref):
    levels, size = loss_ref.shape[0], loss_ref.shape[1]
    inner = levels - 1
    on_diag = eye_of(size)
    top_link, inner_link = top_ref[0:1, 0:1], jnp.full((1, 1), links_ref[inner - 1])
    links = [jnp.full((1, 1), links_ref[k]) for k in range(levels)]

    def diag_of(k):
        above = top_link if k == 0 else links[k - 1]
        return loss_ref[k] + jnp.where(on_diag, 1.0 + above + links[k], 0.0)

    def low(k, x, transposed=False, right=False):
        return links_ref[k - 1] * x

    floor_diag = [
        LEAST + links[k] + (top_link if k == 0 else links[k - 1]) for k in range(levels)
    ]
    panels, thin = dense_inverse(
        [diag_of(k) for k in range(inner)], low, floor_diag[:inner], [top_link] + links[: inner - 1]
    )
    for k, panel in enumerate(panels):
        high, rest = split(panel)
        high_ref[:, k * size : (k + 1) * size] = high
        low_ref[:, k * size : (k + 1) * size] = rest
    ends_ref[0] = top_link * panels[0]
    ends_ref[1] = inner_link * panels[-1]
    blocks = [
        (
            diag_of(inner) - inner_link * inner_link * panels[-1][-size:],
            floor_diag[inner] - inner_link * inner_link * thin[-1][-1],
        ),
        (top_link * top_link * panels[0][:size], top_link * top_link * thin[0][0]),
        (inner_link * top_link * panels[0][-size:], inner_link * top_link * thin[0][-1]),
    ]
    for k, (block, floor) in enumerate(blocks):
        send_ref[k, :size] = block
        send_ref[k, size:] = jnp.broadcast_to(floor, (8, size))


def interface(all_ref, ends_ref, high_ref, low_ref, rows_ref):
    count, size = all_ref.shape[0], all_ref.shape[3]

    def diag_of(rows, cols):
        own = [all_ref[k, 0, rows, cols] for k in range(count)]
        return [
            own[k] - all_ref[k + 1, 1, rows, cols] if k + 1 < count else own[k]
            for k in range(count)
        ]

    def low(k, x, transposed=False, right=False):
        block = all_ref[k, 2, :size]
        if right:
            return dot_t(x, block) if transposed else dot(x, block)
        return dot(block, x, ((0,), (0,))) if transposed else dot(block, x)

    thin = slice(size, size + 1), slice(0, 1)
    panels, _ = dense_inverse(
        diag_of(slice(0, size), slice(0, size)),
        low,
        diag_of(*thin),
        [all_ref[k, 2, thin[0], thin[1]] for k in range(count)],
        enough_steps(spread(size)),
    )
    for k, panel in enumerate(panels):
        rows_ref[k] = panel
    me = lax.axis_index("lev")
    own = rows_ref[me]
    above = rows_ref[jnp.maximum(me - 1, 0)]
    inner = dot_t(ends_ref[0], above) + dot_t(ends_ref[1], own)
    length = inner.shape[0]
    high_ref[:length], low_ref[:length] = split(inner)
    high_ref[length:], low_ref[length:] = split(own.T)


def send(src, dst, sems, slot, device):
    return pltpu.make_async_remote_copy(
        src_ref=src,
        dst_ref=dst,
        send_sem=sems.at[0, slot],
        recv_sem=sems.at[1, slot],
        device_id=device,
        device_id_type=pl.DeviceIdType.MESH,
    )


def greet(lev_all, lon_all):
    barrier = pltpu.get_barrier_semaphore()
    partners = []
    for axis, everyone in (("lev", lev_all), ("lon", lon_all)):
        count, me = lax.axis_size(axis), lax.axis_index(axis)
        if everyone is None:
            continue
        steps = range(1, count) if everyone else sorted({1, count - 1})
        partners += [{axis: lax.rem(me + d, count)} for d in steps if d % count]
    for device in partners:
        pl.semaphore_signal(
            barrier, inc=1, device_id=device, device_id_type=pl.DeviceIdType.MESH
        )
    pl.semaphore_wait(barrier, len(partners))


def pack_edges(cur_ref, edges_ref):
    levels, size, columns = cur_ref.shape
    lane = lax.broadcasted_iota(jnp.int32, (size, 128), 1)
    last = jnp.zeros((size, 128), jnp.float32)
    first = last
    for k in range(levels):
        tail = pltpu.roll(cur_ref[k, :, columns - 128 :], k + 1, 1)
        head = cur_ref[k, :, :128]
        head = pltpu.roll(head, k, 1) if k else head
        last = jnp.where(lane == k, tail, last)
        first = jnp.where(lane == k, head, first)
    edges_ref[0] = last
    edges_ref[1] = first


def halo_copies(edges_ref, halo_ref, sems):
    around, me = lax.axis_size("lon"), lax.axis_index("lon")
    return [
        send(edges_ref.at[0], halo_ref.at[0], sems, 0, {"lon": lax.rem(me + 1, around)}),
        send(edges_ref.at[1], halo_ref.at[1], sems, 1, {"lon": lax.rem(me + around - 1, around)}),
    ]


def local_forcing(mix_ref, cur_ref, prev_ref, pair_ref, force_ref):
    levels, size, columns = cur_ref.shape
    lane = lax.broadcasted_iota(jnp.int32, (size, columns), 1)
    for k in range(levels):
        c = cur_ref[k]
        back = jnp.where(lane == 0, 0.0, pltpu.roll(c, 1, 1))
        ahead = jnp.where(lane == columns - 1, 0.0, pltpu.roll(c, columns - 1, 1))
        p_high, p_low = split(pair_ref[k])
        chem = dot3(p_high, p_low, c * c)
        force_ref[k * size : (k + 1) * size] = (
            prev_ref[k] - chem + mix_ref[k] * (back + ahead - 2.0 * c)
        )


def add_halo(mix_ref, halo_ref, force_ref):
    levels = mix_ref.shape[0]
    size, columns = halo_ref.shape[1], force_ref.shape[1]
    lane = lax.broadcasted_iota(jnp.int32, (size, 128), 1)
    before, after = halo_ref[0], halo_ref[1]
    for k in range(levels):
        rows = slice(k * size, (k + 1) * size)
        at_head = pltpu.roll(before, 128 - k, 1) if k else before
        at_tail = pltpu.roll(after, 127 - k, 1)
        force_ref[rows, :128] += jnp.where(lane == 0, mix_ref[k] * at_head, 0.0)
        force_ref[rows, columns - 128 :] += jnp.where(lane == 127, mix_ref[k] * at_tail, 0.0)


def couple(
    links_ref, top_link, g_high, g_low, force_ref, part_ref, f_high, f_low, top_out, top_in, sides_ref,
    sems, direct,
):
    count, me = lax.axis_size("lev"), lax.axis_index("lev")
    inner, size = part_ref.shape[0], top_out.shape[0]
    f_high[...], f_low[...] = split(force_ref[:inner])
    mul = functools.partial(jnp.dot, preferred_element_type=jnp.float32)

    def rows_of(start, stop):
        a, b = g_high[start:stop], g_low[start:stop]
        part = mul(a, f_high[...]) + (mul(b, f_high[...]) + mul(a, f_low[...]))
        part_ref[start:stop] = part
        return part

    top_out[...] = top_link * rows_of(0, size)
    sides_ref[me] = force_ref[inner:] + links_ref[inner // size - 1] * rows_of(inner - size, inner)
    up = send(top_out, top_in, sems, 0, {"lev": lax.rem(me + count - 1, count)})
    half = size * ((inner // size) // 2)

    @pl.when(me > 0)
    def _():
        up.start()

    rows_of(size, half)

    @pl.when(me < count - 1)
    def _():
        up.wait_recv()
        sides_ref[me] += top_in[...]

    partner = me + 1 - 2 * lax.rem(me, 2)
    copies = [
        send(sides_ref.at[me], sides_ref.at[me], sems, d, {"lev": lax.rem(me + d, count)})
        for d in range(1 if direct else 2, count, 1 if direct else 2)
    ]
    onward = [] if direct else [send(sides_ref.at[me], sides_ref.at[me], sems, 1, {"lev": partner})]
    for d in range(count if direct else 2, count, 2):
        origin = lax.rem(me - d + count, count)
        onward.append(
            send(sides_ref.at[origin], sides_ref.at[origin], sems, d + 1, {"lev": partner})
        )
    for copy in copies + onward[:1]:
        copy.start()
    rows_of(half, inner - size)

    @pl.when(me > 0)
    def _():
        up.wait_send()

    return copies, onward


def relay(copies, onward):
    for copy, later in zip(copies, onward[1:]):
        copy.wait_recv()
        later.start()
    for copy in copies:
        copy.wait_send()
    for copy in onward:
        copy.wait()


def finish(part_ref, sides_ref, high_ref, low_ref, out_ref):
    levels, size, columns = out_ref.shape
    count = sides_ref.shape[0]
    b_high, b_low = split(sides_ref[...].reshape(count * size, columns))
    mul = functools.partial(jnp.dot, preferred_element_type=jnp.float32)
    for k in range(levels):
        rows = slice(k * size, (k + 1) * size)
        a, b = high_ref[rows], low_ref[rows]
        row = mul(a, b_high) + (mul(b, b_high) + mul(a, b_low))
        out_ref[k] = row + part_ref[rows] if k < levels - 1 else row


def open_kernel(
    links_ref, mix_ref, prev_ref, pair_ref, force_ref, top_ref, edges, halo, link_out, sems
):
    levels = prev_ref.shape[0]
    count, me = lax.axis_size("lev"), lax.axis_index("lev")
    pack_edges(prev_ref, edges)
    link_out[...] = jnp.full(link_out.shape, links_ref[levels - 1], jnp.float32)
    greet(False, False)
    copies = halo_copies(edges, halo, sems)
    down = send(link_out, top_ref, sems, 2, {"lev": lax.rem(me + 1, count)})
    for copy in copies:
        copy.start()

    @pl.when(me < count - 1)
    def _():
        down.start()

    @pl.when(me == 0)
    def _():
        top_ref[...] = jnp.zeros(top_ref.shape, jnp.float32)

    local_forcing(mix_ref, prev_ref, prev_ref, pair_ref, force_ref)
    for copy in copies:
        copy.wait()
    add_halo(mix_ref, halo, force_ref)

    @pl.when(me < count - 1)
    def _():
        down.wait_send()

    @pl.when(me > 0)
    def _():
        down.wait_recv()


def newton_kernel(
    links_ref, mix_ref, top_ref, sent_ref, ends_ref, first_force, g_high, g_low, prev_ref, pair_ref,
    out_ref, var_ref, all_ref, rows_ref, h_high, h_low, cur_ref, edges, halo, force_ref, part_ref,
    first_sides, sides_ref, f_high, f_low, first_out, first_in, top_out, top_in, sums_ref,
    block_sems, first_sems, halo_sems, sems, sum_sems,
):
    levels, size, columns = prev_ref.shape
    count, me = lax.axis_size("lev"), lax.axis_index("lev")
    around, place = lax.axis_size("lon"), lax.axis_index("lon")
    greet(True, True)
    blocks = [
        send(sent_ref, all_ref.at[me], block_sems, d, {"lev": lax.rem(me + d, count)})
        for d in range(1, count)
    ]
    for copy in blocks:
        copy.start()
    all_ref[me] = sent_ref[...]
    copies = couple(
        links_ref, top_ref[0:1, 0:1], g_high, g_low, first_force, part_ref, f_high, f_low,
        first_out, first_in, first_sides, first_sems, True,
    )
    for copy in blocks:
        copy.wait()
    interface(all_ref, ends_ref, h_high, h_low, rows_ref)
    for copy in copies[0]:
        copy.wait()
    finish(part_ref, first_sides, h_high, h_low, cur_ref)
    pack_edges(cur_ref, edges)
    copies = halo_copies(edges, halo, halo_sems)
    for copy in copies:
        copy.start()
    local_forcing(mix_ref, cur_ref, prev_ref, pair_ref, force_ref)
    for copy in copies:
        copy.wait()
    add_halo(mix_ref, halo, force_ref)
    copies = couple(
        links_ref, top_ref[0:1, 0:1], g_high, g_low, force_ref, part_ref, f_high, f_low,
        top_out, top_in, sides_ref, sems, False,
    )
    relay(*copies)
    finish(part_ref, sides_ref, h_high, h_low, out_ref)
    lane = lax.broadcasted_iota(jnp.int32, (size, 128), 1)
    total = jnp.zeros((size, 128), jnp.float32)
    for k in range(levels):
        row = out_ref[k]
        total = jnp.where(lane == k, jnp.sum(row * row, axis=1, keepdims=True), total)
    sums_ref[0] = total.T[: sums_ref.shape[1]]
    copies = [
        send(sums_ref.at[0], sums_ref.at[d], sum_sems, d, {"lon": lax.rem(place + d, around)})
        for d in range(1, around)
    ]
    for copy in copies:
        copy.start()
    for copy in copies:
        copy.wait()
    total = sums_ref[place]
    for j in range(1, around):
        total = total + sums_ref[lax.rem(place - j + around, around)]
    var_ref[...] = (total / (columns * around))[:levels]


def call(kernel, outs, places, scratch=(), group=None):
    extra = {} if group is None else {"collective_id": group, "has_side_effects": True}
    return pl.pallas_call(
        kernel,
        out_shape=[jax.ShapeDtypeStruct(shape, dtype) for shape, dtype in outs],
        in_specs=places,
        out_specs=[VMEM] * len(outs),
        scratch_shapes=list(scratch),
        compiler_params=pltpu.CompilerParams(vmem_limit_bytes=60 * 2**20, **extra),
    )


def local(previous, loss_matrix, pair_matrix, diffusivity, mixing):
    levels, size, columns = previous.shape
    count = lax.axis_size("lev")
    around = lax.axis_size("lon")
    inner = (levels - 1) * size
    f32, bf16 = jnp.float32, jnp.bfloat16
    buf, sem = pltpu.VMEM, lambda n: pltpu.SemaphoreType.DMA((2, n))
    force, top = call(
        open_kernel,
        [((levels * size, columns), f32), ((8, 128), f32)],
        [SMEM, SMEM, VMEM, VMEM],
        [buf((2, size, 128), f32), buf((2, size, 128), f32), buf((8, 128), f32), sem(3)],
        0,
    )(diffusivity, mixing, previous, pair_matrix)
    g_high, g_low, ends, sent = call(
        factor_kernel,
        [((inner, inner), bf16), ((inner, inner), bf16), ((2, inner, size), f32), ((3, size + 8, size), f32)],
        [SMEM, VMEM, VMEM],
    )(diffusivity, top, loss_matrix)
    return call(
        newton_kernel,
        [((levels, size, columns), f32), ((levels, size), f32)],
        [SMEM, SMEM] + [VMEM] * 8,
        [
            buf((count, 3, size + 8, size), f32),
            buf((count, count * size, size), f32),
            buf((levels * size, count * size), bf16),
            buf((levels * size, count * size), bf16),
            buf((levels, size, columns), f32),
            buf((2, size, 128), f32),
            buf((2, size, 128), f32),
            buf((levels * size, columns), f32),
            buf((inner, columns), f32),
            buf((count, size, columns), f32),
            buf((count, size, columns), f32),
            buf((inner, columns), bf16),
            buf((inner, columns), bf16),
            buf((size, columns), f32),
            buf((size, columns), f32),
            buf((size, columns), f32),
            buf((size, columns), f32),
            buf((around, -(-levels // 8) * 8, size), f32),
            sem(count),
            sem(count),
            sem(2),
            sem(count),
            sem(around),
        ],
        1,
    )(diffusivity, mixing, top, sent, ends, force, g_high, g_low, previous, pair_matrix)


def solution(mesh):
    placed = (P("lev", None, "lon"), P("lev", None, None), P("lev", None, None), P("lev"), P("lev"))
    return jax.shard_map(
        local,
        mesh=mesh,
        in_specs=placed,
        out_specs=(P("lev", None, "lon"), P("lev", None)),
        check_vma=False,
    )
```
